128 devices in a mesh: tm: 64 (over y, x, z), batch: 2 (over core).
Axes of the slice: x: 4, y: 4, z: 4, core: 2. Of those that a mesh axis runs over, the one named last changes fastest.
Arguments:
- state_map: float32 [2048, 256, 256], P(('batch', 'tm')), parts along dimension 0, may hold values from -0.375 to 0.375
- input_map: float32 [2048, 64, 256], P(('batch', 'tm')), parts along dimension 0, may hold values from -0.375 to 0.375
- closed_loop: float32 [2048, 256, 256], P(('batch', 'tm')), parts along dimension 0, may hold values from -1.001 to 1.001
- feedback: float32 [2048, 64, 256], P(('batch', 'tm')), parts along dimension 0, may hold values from -0.375 to 0.375
- value_matrix: float32 [2048, 256, 256], P(('batch', 'tm')), parts along dimension 0, may hold values from -0.046875 to 1.5, as said below
- gain_inverse: float32 [2048, 64, 64], P(('batch', 'tm')), parts along dimension 0, may hold values from -0.0105 to 0.2, as said below
- input_weight: float32 [128, 64], P('batch'), parts along dimension 0, may hold values from -0.36 to 6, as said below
- state_weight: float32 [2048, 256], P(('batch', 'tm')), parts along dimension 0, may hold values from 0.1 to 3
- state_linear: float32 [2048, 256], P(('batch', 'tm')), parts along dimension 0, may hold values from -0.18 to 0.18
- input_linear: float32 [2048, 64], P(('batch', 'tm')), parts along dimension 0, may hold values from -0.18 to 0.18
- offset: float32 [2048, 256], P(('batch', 'tm')), parts along dimension 0, may hold values from -0.18 to 0.18
- upper_bound: float32 [2048, 64], P(('batch', 'tm')), parts along dimension 0, may hold values from 0.1 to 0.3
- states: float32 [2048, 256], P(('batch', 'tm')), parts along dimension 0, may hold values from -0.18 to 0.18
- inputs: float32 [2048, 64], P(('batch', 'tm')), parts along dimension 0, may hold values from -0.18 to 0.18
- multipliers: float32 [2048, 256], P(('batch', 'tm')), parts along dimension 0, may hold values from -0.18 to 0.18
- bound_mult: float32 [2048, 64], P(('batch', 'tm')), parts along dimension 0, may hold values from 0 to 0.06
- active: int32 [2048, 64], P(('batch', 'tm')), parts along dimension 0, may hold values 0 or 1
Outputs:
- state_step: float32 [2048, 256], P(('batch', 'tm')), parts along dimension 0
- input_step: float32 [2048, 64], P(('batch', 'tm')), parts along dimension 0
- multiplier_step: float32 [2048, 256], P(('batch', 'tm')), parts along dimension 0
- bound_step: float32 [2048, 64], P(('batch', 'tm')), parts along dimension 0
- kkt_norms: float32 [6], P('batch'), parts along dimension 0
The draws below stay inside these ranges and needn't reach their ends.
There are 2 independent parts, one for each index of `batch`. The reference program is written for one: setup_inputs(seed, part) draws one part's arguments, and reference() takes and returns one part's arrays. A program takes and returns all parts, laid end to end along the dimension named above; each array names one. Nothing has to cross between parts.
Inputs may be any that keep to these rules, and one draw needn't show every extreme that they name: `value_matrix`: each section's matrix is symmetric. `gain_inverse`: each section's matrix is symmetric. `input_weight`: symmetric.
All inputs are finite; a program needn't handle non-finite values. No bound on the sum of `active` on one device may be relied on, other than what follows from the above.
Results may differ from the reference program's by a relative error of at most 0.0003.
Values sent between devices are 32-bit elements; how exact they have to be, the bound alone decides.
No kernel may reach another device: no remote copies, remote signals or barrier semaphores. Data moves between devices by JAX's collectives and lax.ppermute only.
A program may use at most 128 MiB of HBM per device.

```python
import math
import jax
import jax.numpy as jnp
from jax import lax

NS = 256
NU = 64
HORIZON = 1024


def symmetric_draw(key, sections, dimension, lowest, highest, spread):
    first_key, second_key = jax.random.split(key)
    diagonal = jax.random.uniform(first_key, (sections, dimension), jnp.float32, lowest, highest)
    noise_raw = jax.random.normal(second_key, (sections, dimension, dimension), jnp.float32) * spread
    mixed = jnp.clip((noise_raw + jnp.swapaxes(noise_raw, 1, 2)) / math.sqrt(2.0), -3.0 * spread, 3.0 * spread)
    identity = jnp.eye(dimension, dtype=jnp.float32)
    return mixed * (1.0 - identity) + diagonal[:, :, None] * identity


def draw_value_matrix(key, part):
    return symmetric_draw(jax.random.fold_in(key, 11), HORIZON, NS, 0.5, 1.5, 0.25 / math.sqrt(NS))


def draw_gain_inverse(key, part):
    return symmetric_draw(jax.random.fold_in(key, 12), HORIZON, NU, 0.08, 0.2, 0.028 / math.sqrt(NU))


def draw_input_weight(key, part):
    return symmetric_draw(jax.random.fold_in(key, 13), 1, NU, 2.0, 6.0, 0.96 / math.sqrt(NU))[0]


def draw_closed_loop(key, part):
    subkeys = jax.random.split(jax.random.fold_in(key, 7), 5)
    ranking = jax.random.permutation(subkeys[0], NS)
    slow_total = NS // 2
    slow_channel = ranking < slow_total
    same_class = (slow_channel[:, None] == slow_channel[None, :]).astype(jnp.float32)
    slow_rate = jax.random.uniform(subkeys[1], (HORIZON, NS), jnp.float32, 0.3, 2.0) / HORIZON
    memory = jnp.exp(jax.random.uniform(subkeys[2], (HORIZON, NS), jnp.float32, math.log(2.0), math.log(8.0)))
    decays = jnp.where(slow_channel[None, :], jnp.exp(-slow_rate), jnp.exp(-1.0 / memory))
    noise_raw = jax.random.normal(subkeys[3], (HORIZON, NS, NS), jnp.float32) * (0.5 / math.sqrt(NS))
    cross_raw = jax.random.normal(subkeys[4], (HORIZON, NS, NS), jnp.float32) * (0.25 / math.sqrt(NS * HORIZON))
    within_part = (noise_raw - jnp.swapaxes(noise_raw, 1, 2)) * same_class
    between_part = (cross_raw - jnp.swapaxes(cross_raw, 1, 2)) * (1.0 - same_class)
    skew_part = within_part + between_part
    identity = jnp.eye(NS, dtype=jnp.float32)
    rotation = jnp.linalg.solve(identity + skew_part, identity - skew_part)
    return decays[:, :, None] * rotation


def with_ends(array, stream_key, low, top_value):
    spot = [jax.random.randint(jax.random.fold_in(stream_key, axis), (), 0, length) for axis, length in enumerate(array.shape)]
    main_axis = array.shape.index(max(array.shape))
    next_to = spot[:main_axis] + [(spot[main_axis] + 1) % array.shape[main_axis]] + spot[main_axis + 1:]
    return array.at[tuple(spot)].set(low).at[tuple(next_to)].set(top_value)


def block_scale(key, dims, shards, low, high):
    level = 1.0
    for axis_at, blocks in shards:
        draws = jax.random.uniform(jax.random.fold_in(jax.random.fold_in(key, 6), axis_at), (blocks,), jnp.float32, low / len(shards), high / len(shards))
        level = level * jnp.repeat(jnp.exp(draws), dims[axis_at] // blocks).reshape((-1,) + (1,) * (len(dims) - 1 - axis_at))
    return level


def noise(own_key, shape, scale, limit, cuts=(), kind=jnp.bfloat16):
    drawn = jax.random.normal(own_key, shape, jnp.float32) * scale
    if len(cuts) > 0:
        drawn = block_scale(own_key, shape, cuts, -0.22, 0.18) * drawn
    return jnp.clip(drawn, min=-limit, max=limit).astype(kind)


def setup_inputs(seed: int = 0, part: int = 0) -> dict:
    key_list = jax.random.split(jax.random.key(seed), 18)
    part_splits = jax.random.split(jax.random.fold_in(key_list[17], part), 18)
    state_map = noise(part_splits[0], (HORIZON, NS, NS), NS ** -0.5, 0.375, ((0, 64),), jnp.float32)
    input_map = noise(part_splits[1], (HORIZON, NU, NS), NS ** -0.5, 0.375, ((0, 64),), jnp.float32)
    closed_loop = draw_closed_loop(jax.random.fold_in(jax.random.fold_in(key_list[17], part), 71), part)
    feedback = noise(part_splits[3], (HORIZON, NU, NS), NS ** -0.5, 0.375, ((0, 64),), jnp.float32)
    value_matrix = draw_value_matrix(jax.random.fold_in(jax.random.fold_in(key_list[17], part), 71), part)
    gain_inverse = draw_gain_inverse(jax.random.fold_in(jax.random.fold_in(key_list[17], part), 71), part)
    input_weight = draw_input_weight(jax.random.fold_in(jax.random.fold_in(key_list[17], part), 71), part)
    state_weight = jnp.clip(jnp.exp(math.log(3.0) - 3.4011974 * jax.random.uniform(part_splits[7], (HORIZON, NS), jnp.float32) ** block_scale(part_splits[7], (HORIZON, NS), ((0, 64),), -0.2, 0.2)), 0.1, 3.0)
    state_linear = noise(part_splits[8], (HORIZON, NS), 0.03, 0.18, ((0, 64),), jnp.float32)
    input_linear = noise(part_splits[9], (HORIZON, NU), 0.03, 0.18, ((0, 64),), jnp.float32)
    offset = noise(part_splits[10], (HORIZON, NS), 0.03, 0.18, ((0, 64),), jnp.float32)
    upper_bound = jnp.clip(0.1 + 0.20000001043081284 * jax.random.uniform(part_splits[11], (HORIZON, NU), jnp.float32) ** block_scale(part_splits[11], (HORIZON, NU), ((0, 64),), -0.2, 0.2), 0.1, 0.3)
    states = noise(part_splits[12], (HORIZON, NS), 0.03, 0.18, ((0, 64),), jnp.float32)
    inputs = noise(part_splits[13], (HORIZON, NU), 0.03, 0.18, ((0, 64),), jnp.float32)
    multipliers = noise(part_splits[14], (HORIZON, NS), 0.03, 0.18, ((0, 64),), jnp.float32)
    bound_mult = jnp.clip(0.06 * jax.random.uniform(part_splits[15], (HORIZON, NU), jnp.float32) ** block_scale(part_splits[15], (HORIZON, NU), ((0, 64),), -0.2, 0.2), 0.0, 0.06)
    active = with_ends((jax.random.randint(part_splits[16], (HORIZON, NU), 0, 3) < 1).astype(jnp.int32), jax.random.fold_in(part_splits[16], 1), 0, 1)
    return dict(state_map=state_map, input_map=input_map, closed_loop=closed_loop, feedback=feedback, value_matrix=value_matrix, gain_inverse=gain_inverse, input_weight=input_weight, state_weight=state_weight, state_linear=state_linear, input_linear=input_linear, offset=offset, upper_bound=upper_bound, states=states, inputs=inputs, multipliers=multipliers, bound_mult=bound_mult, active=active)


PRECISE = lax.Precision.HIGHEST
floor_share = 0.001

def apply_each(matrices, vectors):
    return jnp.einsum('kij,kj->ki', matrices, vectors, precision=PRECISE)

def apply_transposed(matrices, vectors):
    return jnp.einsum('kji,kj->ki', matrices, vectors, precision=PRECISE)

def backward_sweep(loop_mats, sources, incoming):

    def section(costate, section_item):
        matrix, source = section_item
        earlier = jnp.dot(costate, matrix, precision=PRECISE) + source
        return (earlier, (costate, earlier))
    final_state, (after, before) = lax.scan(section, incoming, (loop_mats, sources), reverse=True)
    return (after, before, final_state)

def forward_sweep(loop_mats, defects, pushes, entering):

    def section(carried, section_item):
        matrix, defect, pushed = section_item
        correction = carried - defect
        return (jnp.dot(matrix, correction, precision=PRECISE) + pushed, correction)
    final_state, steps = lax.scan(section, entering, (loop_mats, defects, pushes))
    return (steps, final_state)

def make_statistics(defect, grad_state, grad_input, slack_gap, offset, state_linear, input_linear, bound_mult):
    return jnp.stack([jnp.sum(defect * defect), jnp.sum(grad_state * grad_state) + jnp.sum(grad_input * grad_input), jnp.sum(slack_gap * slack_gap), jnp.sum(offset * offset), jnp.sum(state_linear * state_linear) + jnp.sum(input_linear * input_linear), jnp.sum(bound_mult * bound_mult)])

def make_norms(totals, horizon, state_count, input_count):
    primal = totals[0] / (totals[3] + floor_share * horizon * state_count)
    dual = totals[1] / (totals[4] + floor_share * horizon * (state_count + input_count))
    complement = totals[2] / (totals[5] + floor_share * horizon * input_count)
    return jnp.sqrt(jnp.stack([primal, dual, complement]))

def reference(state_map, input_map, closed_loop, feedback, value_matrix, gain_inverse, input_weight, state_weight, state_linear, input_linear, offset, upper_bound, states, inputs, multipliers, bound_mult, active):
    state_count = states.shape[1]
    input_count = inputs.shape[1]
    horizon = states.shape[0]
    predicted = apply_each(state_map, states) + apply_transposed(input_map, inputs)
    previous = jnp.concatenate([jnp.zeros((1, state_count), jnp.float32), predicted[:-1]], axis=0)
    defect = states - previous - offset
    following = jnp.concatenate([multipliers[1:], jnp.zeros((1, state_count), jnp.float32)], axis=0)
    grad_state = state_weight * states + state_linear + multipliers - apply_transposed(state_map, following)
    grad_input = jnp.einsum('ij,kj->ki', input_weight, inputs, precision=PRECISE) + input_linear - apply_each(input_map, following) + bound_mult
    slack_gap = bound_mult * (upper_bound - inputs)
    sources = apply_each(value_matrix, defect) + grad_state + apply_transposed(feedback, grad_input)
    after, before, unused = backward_sweep(closed_loop, sources, jnp.zeros((state_count,), jnp.float32))
    pulled = apply_each(input_map, after)
    forward_gain = -apply_each(gain_inverse, grad_input + pulled)
    pushes = apply_transposed(input_map, forward_gain)
    state_step, unused_final = forward_sweep(closed_loop, defect, pushes, jnp.zeros((state_count,), jnp.float32))
    chosen = active.astype(jnp.float32)
    input_step = (1.0 - chosen) * (apply_each(feedback, state_step) + forward_gain) + chosen * (upper_bound - inputs)
    multiplier_step = apply_each(value_matrix, state_step - defect) + before
    bound_step = chosen * (grad_input + jnp.einsum('ij,kj->ki', input_weight, input_step, precision=PRECISE) + pulled)
    totals = make_statistics(defect, grad_state, grad_input, slack_gap, offset, state_linear, input_linear, bound_mult)
    kkt_norms = make_norms(totals, horizon, state_count, input_count)
    return (state_step, input_step, multiplier_step, bound_step, kkt_norms)
```

```python
import functools

import jax
import jax.numpy as jnp
from jax import lax
from jax.experimental import pallas as pl
from jax.experimental.pallas import tpu as pltpu
from jax.sharding import Mesh
from jax.sharding import PartitionSpec as P

TM = ("tm_0", "tm_1", "tm_2")
BATCH_TM = ("batch", "tm_0", "tm_1", "tm_2")
F32 = jnp.float32
BF16 = jnp.bfloat16
floor_share = 0.001
VMEM = pltpu.VMEM
SMEM = pltpu.SMEM


def halves(x):
    high = x.astype(BF16)
    low = (x - high.astype(F32)).astype(BF16)
    return high, low


def dot(a, b, ca, cb):
    return lax.dot_general(a, b, (((ca,), (cb,)), ((), ())), preferred_element_type=F32)


def mat_mul(a, b, ca=1, cb=0):
    ah, al = halves(a)
    bh, bl = halves(b)
    return dot(ah, bh, ca, cb) + (dot(ah, bl, ca, cb) + dot(al, bh, ca, cb))


def row_halves(v):
    high = v.astype(BF16).astype(F32)
    row = lax.broadcasted_iota(jnp.int32, (8, v.shape[1]), 0)
    both = jnp.where(row == 0, high, jnp.where(row == 1, v - high, 0.0))
    return both.astype(BF16)


def vec_mat(v, m, cb=0):
    lhs = row_halves(v)
    mh, ml = halves(m)
    r = dot(lhs, mh, 1, cb) + dot(lhs, ml, 1, cb)
    return jnp.sum(r, axis=0, keepdims=True)


def last_prediction_body(ready, f_ref, m_ref, x_ref, u_ref, out_ref):
    ready(0)
    v = vec_mat(x_ref[7:8, :], f_ref[0], 1) + vec_mat(u_ref[7:8, :], m_ref[0])
    out_ref[...] = jnp.broadcast_to(v, (8, 256))


def block_product_body(ready, a_ref, p_ref, pair_ref, quad_ref, half_ref):
    for j in range(4):
        ready(j)
        low = mat_mul(a_ref[4 * j + 1], a_ref[4 * j])
        high = mat_mul(a_ref[4 * j + 3], a_ref[4 * j + 2])
        pair_ref[j] = high
        quad_ref[j] = mat_mul(high, low)
        if j == 1:
            half_ref[...] = mat_mul(quad_ref[1], quad_ref[0])
    p_ref[...] = mat_mul(mat_mul(quad_ref[3], quad_ref[2]), half_ref[...])


def total(x):
    return jnp.sum(jnp.sum(x, axis=0, keepdims=True), axis=1, keepdims=True)


def sources_body(
    ready, f_ref, m_ref, v_ref, k_ref, a_ref,
    x_ref, u_ref, mult_ref, bm_ref, ub_ref, off_ref, sw_ref, sl_ref, il_ref, iw_ref,
    quad_ref, half_ref, before_ref, next_ref,
    defect_ref, gi_ref, src_ref, b_ref, c_ref, stat_ref,
    gs_ref,
):
    gi_ref[...] = mat_mul(u_ref[...], iw_ref[...], 1, 1) + il_ref[...] + bm_ref[...]
    gs_ref[...] = sw_ref[...] * x_ref[...] + sl_ref[...] + mult_ref[...]
    src_ref[...] = x_ref[...] - off_ref[...]
    prev = before_ref[0:1, :]
    for i in range(4):
        ready(i)
        for j in range(4):
            k = i * 4 + j
            follow = next_ref[0:1, :] if k == 15 else mult_ref[k + 1:k + 2, :]
            gs = gs_ref[k:k + 1, :] - vec_mat(follow, f_ref[k])
            gs_ref[k:k + 1, :] = gs
            gi = gi_ref[k:k + 1, :] - vec_mat(follow, m_ref[k], 1)
            gi_ref[k:k + 1, :] = gi
            d = src_ref[k:k + 1, :] - prev
            defect_ref[k:k + 1, :] = d
            src_ref[k:k + 1, :] = vec_mat(d, v_ref[k]) + gs + vec_mat(gi, k_ref[k])
            if k < 15:
                prev = vec_mat(x_ref[k:k + 1, :], f_ref[k], 1) + vec_mat(u_ref[k:k + 1, :], m_ref[k])
    b = [src_ref[4 * j + 3:4 * j + 4, :] for j in range(4)]
    for j in range(4):
        b_ref[4 * j + 3:4 * j + 4, :] = b[j]
    for m in (2, 1, 0):
        for j in range(4):
            k = 4 * j + m
            b[j] = vec_mat(b[j], a_ref[k]) + src_ref[k:k + 1, :]
            b_ref[k:k + 1, :] = b[j]
    upper = b[2] + vec_mat(b[3], quad_ref[2])
    c = b[0] + vec_mat(b[1], quad_ref[0]) + vec_mat(upper, half_ref[...])
    c_ref[...] = jnp.broadcast_to(c, (8, 256))

    gap = bm_ref[...] * (ub_ref[...] - u_ref[...])
    d, gs, gi = defect_ref[...], gs_ref[...], gi_ref[...]
    off, sl, il, bm = off_ref[...], sl_ref[...], il_ref[...], bm_ref[...]
    found = (
        total(d * d),
        total(gs * gs) + total(gi * gi),
        total(gap * gap),
        total(off * off),
        total(sl * sl) + total(il * il),
        total(bm * bm),
    )
    lane = lax.broadcasted_iota(jnp.int32, (8, 128), 1)
    out = jnp.zeros((8, 128), F32)
    for n, s in enumerate(found):
        out = jnp.where(lane == n, s, out)
    stat_ref[...] = out


def weight_body(ready, a_ref, m_ref, g_ref, pair_ref, quad_ref, half_ref, w_ref, third_ref, b_ref, gb_ref):
    third_ref[...] = mat_mul(quad_ref[2], half_ref[...])
    ready(0)
    for j in range(4):
        k = 4 * j
        r = 256 * j
        b_ref[r:r + 64, :] = mat_mul(m_ref[k], a_ref[k + 1], 1, 1)
        b_ref[r + 64:r + 128, :] = m_ref[k + 1]
        b_ref[r + 128:r + 192, :] = mat_mul(m_ref[k + 2], a_ref[k + 3], 1, 1)
        b_ref[r + 192:r + 256, :] = m_ref[k + 3]
        b_ref[r:r + 128, :] = mat_mul(b_ref[r:r + 128, :], pair_ref[j], 1, 1)
    for j in (1, 2, 3):
        b_ref[0:256 * j, :] = mat_mul(b_ref[0:256 * j, :], quad_ref[j], 1, 1)
    for k in range(16):
        gb_ref[64 * k:64 * k + 64, :] = mat_mul(g_ref[k], b_ref[64 * k:64 * k + 64, :])
    w_ref[...] = mat_mul(b_ref[...], gb_ref[...], 0, 0)


def sweep_body(
    ready, a_ref, m_ref, g_ref, *refs,
):
    quad_ref, b_ref, src_ref, gi_ref, defect_ref = refs[:5]
    lam_ref = refs[5] if len(refs) > 12 else None
    before_ref, gain_ref, base_ref, push_ref, entry_ref, end_ref, after_ref = refs[-7:]
    lams = [None, None, None, jnp.zeros((1, 256), F32) if lam_ref is None else lam_ref[0:1, :]]
    for j in (2, 1, 0):
        lams[j] = vec_mat(lams[j + 1], quad_ref[j + 1]) + b_ref[4 * j + 4:4 * j + 5, :]
    before_ref[0:1, :] = vec_mat(lams[0], quad_ref[0]) + b_ref[0:1, :]
    for j in range(3):
        before_ref[4 * j + 4:4 * j + 5, :] = lams[j]
    ready(0)
    for m in (3, 2, 1, 0):
        for j in range(4):
            k = 4 * j + m
            after_ref[k:k + 1, :] = lams[j]
            if m > 0:
                lams[j] = vec_mat(lams[j], a_ref[k]) + src_ref[k:k + 1, :]
                before_ref[k:k + 1, :] = lams[j]
    for k in range(16):
        base = gi_ref[k:k + 1, :] + vec_mat(after_ref[k:k + 1, :], m_ref[k], 1)
        base_ref[k:k + 1, :] = base
        gain = -vec_mat(base, g_ref[k])
        gain_ref[k:k + 1, :] = gain
        push_ref[k:k + 1, :] = vec_mat(gain, m_ref[k])
    ends = [jnp.zeros((1, 256), F32)] * 4
    for m in range(4):
        for j in range(4):
            k = 4 * j + m
            step = ends[j] - defect_ref[k:k + 1, :]
            ends[j] = vec_mat(step, a_ref[k], 1) + push_ref[k:k + 1, :]
    entry_ref[...] = jnp.zeros_like(entry_ref)
    e = ends[0]
    for j in (1, 2, 3):
        entry_ref[j:j + 1, :] = e
        e = vec_mat(e, quad_ref[j], 1) + ends[j]
    end_ref[...] = jnp.broadcast_to(e, (8, 256))


def order(ref, place, own, minus, plus, across):
    ref[place] = own
    ref[lax.rem(place + 1, 4)] = plus
    ref[lax.rem(place + 2, 4)] = across
    ref[lax.rem(place + 3, 4)] = minus


def join_body(ready, idx_ref, *refs, axis):
    place = idx_ref[axis]
    maps_ref, vectors_ref, out_ref = refs[-3:]
    parts = refs[:4]
    order(maps_ref, place, *[r[0:256, :] for r in parts])
    order(vectors_ref, place, *([r[...] for r in refs[4:8]] if len(refs) > 7 else [r[256:264, :] for r in parts]))
    high = mat_mul(maps_ref[3], maps_ref[2])
    low = mat_mul(maps_ref[1], maps_ref[0])
    v = vectors_ref[3, 0:1, :]
    for j in (2, 1, 0):
        v = vec_mat(v, maps_ref[j]) + vectors_ref[j, 0:1, :]
    out_ref[0:256, :] = mat_mul(high, low)
    out_ref[256:264, :] = jnp.broadcast_to(v, (8, 256))


def chain_back(lam, maps, order, place):
    picked = lam
    for j in (3, 2, 1):
        lam = vec_mat(lam, maps[j]) + order[j, 0:1, :]
        picked = jnp.where(place == j - 1, lam, picked)
    return picked


def costate_body(
    ready, idx_ref, h0_ref, hm_ref, hp_ref, h2_ref,
    gx_ref, cx_ref, pz_ref, cz_ref, w_ref, s0_ref, stat_ref,
    lam_ref, msg_ref, hy_ref, order_ref,
):
    y = idx_ref[0]
    x = idx_ref[1]
    z = idx_ref[2]
    refs = (h0_ref, hm_ref, hp_ref, h2_ref)
    order(hy_ref, y, *[r[0:256, :] for r in refs])
    order(order_ref, y, *[r[256:264, :] for r in refs])
    lam = chain_back(jnp.zeros((1, 256), F32), hy_ref, order_ref, y)
    lam = chain_back(lam, gx_ref, cx_ref, x)
    lam = chain_back(lam, pz_ref, cz_ref, z)
    lam_ref[...] = jnp.broadcast_to(lam, (8, 256))
    s = s0_ref[0:1, :] - vec_mat(lam, w_ref[...])
    u1 = s
    for j in (1, 2, 3):
        s = jnp.where(z + j <= 3, vec_mat(s, pz_ref[jnp.minimum(z + j, 3)], 1), s)
    u2 = s
    for j in (1, 2, 3):
        s = jnp.where(x + j <= 3, vec_mat(s, gx_ref[jnp.minimum(x + j, 3)], 1), s)
    u3 = s
    d = lax.broadcasted_iota(jnp.int32, (64, 256), 0)
    group = lax.shift_right_logical(d, 2)
    plane = lax.shift_right_logical(d, 4)
    msg_ref[:, 0, 0:256] = jnp.where(group == y * 4 + x, u1, jnp.where(plane == y, u2, u3))
    msg_ref[:, 0, 256:384] = jnp.broadcast_to(stat_ref[0:1, :], (64, 128))


def chain_forth(e, maps, sums, place):
    picked = e
    for j in (0, 1, 2):
        e = vec_mat(e, maps[j], 1) + sums[j]
        picked = jnp.where(place == j + 1, e, picked)
    return picked


def finish_body(
    ready, idx_ref, a_ref, v_ref, k_ref, active_ref, ub_ref, u_ref, iw_ref,
    h0_ref, hm_ref, hp_ref, h2_ref, gx_ref, pz_ref, quad_ref, half_ref, third_ref,
    entry_ref, push_ref, defect_ref, before_ref, gain_ref, base_ref, msg_ref,
    ss_ref, is_ref, ms_ref, bs_ref, norm_ref, hy_ref,
    *, horizon,
):
    order(hy_ref, idx_ref[0], *[r[0:256, :] for r in (h0_ref, hm_ref, hp_ref, h2_ref)])
    y = idx_ref[0]
    x = idx_ref[1]
    z = idx_ref[2]
    d = lax.broadcasted_iota(jnp.int32, (64, 256), 0)
    plane = lax.shift_right_logical(d, 4)
    group = lax.shift_right_logical(d, 2)
    msg = msg_ref[:, 0, 0:256]

    def picked(mask):
        return jnp.sum(jnp.where(mask, msg, 0.0), axis=0, keepdims=True)

    e = chain_forth(jnp.zeros((1, 256), F32), hy_ref, [picked(plane == j) for j in range(3)], y)
    e = chain_forth(e, gx_ref, [picked(group == y * 4 + j) for j in range(3)], x)
    e = chain_forth(e, pz_ref, [picked(d == y * 16 + x * 4 + j) for j in range(3)], z)
    sums = jnp.sum(msg_ref[:, 0, 256:384], axis=0, keepdims=True)
    lane = lax.broadcasted_iota(jnp.int32, (1, 128), 1)
    share = floor_share * horizon
    floors = jnp.where(lane == 0, share * 256, jnp.where(lane == 1, share * 320, share * 64))
    norm_ref[...] = jnp.sqrt(sums / (pltpu.roll(sums, 125, 1) + floors))[:, 0:3]
    ends = [
        e,
        vec_mat(e, quad_ref[0], 1) + entry_ref[1:2, :],
        vec_mat(e, half_ref[...], 1) + entry_ref[2:3, :],
        vec_mat(e, third_ref[...], 1) + entry_ref[3:4, :],
    ]
    ready(0)
    for m in range(4):
        for j in range(4):
            k = 4 * j + m
            step = ends[j] - defect_ref[k:k + 1, :]
            ss_ref[k:k + 1, :] = step
            if m < 3:
                ends[j] = vec_mat(step, a_ref[k], 1) + push_ref[k:k + 1, :]
    for k in range(16):
        step = ss_ref[k:k + 1, :]
        ms_ref[k:k + 1, :] = vec_mat(step - defect_ref[k:k + 1, :], v_ref[k]) + before_ref[k:k + 1, :]
        is_ref[k:k + 1, :] = vec_mat(step, k_ref[k], 1) + gain_ref[k:k + 1, :]
    chosen = active_ref[...].astype(F32)
    step = (1.0 - chosen) * is_ref[...] + chosen * (ub_ref[...] - u_ref[...])
    is_ref[...] = step
    bs_ref[...] = chosen * (base_ref[...] + mat_mul(step, iw_ref[...], 1, 1))


def sds(*shape):
    return jax.ShapeDtypeStruct(shape, F32)


SCALARS = pl.BlockSpec(memory_space=SMEM)
FULL = pl.BlockSpec(memory_space=VMEM)


def in_vmem(shape):
    return pltpu.VMEM(shape, F32)


def call(body, scalars, big, small, near, outs, scratch, chunks=1, final=False, away=()):
    ns, nb, nm, nn, no = len(scalars), len(big), len(small), len(near), len(outs)
    far = [b if isinstance(b, tuple) else (b, 0, b.shape[0]) for b in list(big) + list(small)]

    def kernel(*refs):
        refs = list(refs)

        def take(n):
            out = refs[:n]
            del refs[:n]
            return out

        scalar_refs, far_refs, near_refs, out_refs, local_refs = take(ns), take(nb + nm), take(nn), take(no), take(nb + nm)
        sems = refs.pop() if far else None
        moves = [[] for _ in range(chunks)]
        first = []
        n = 0
        for at, ((_, low, size), src, dst) in enumerate(zip(far, far_refs, local_refs)):
            pieces = chunks if at < nb else 1
            step = size // pieces
            for c in range(pieces):
                move = pltpu.make_async_copy(
                    src.at[pl.ds(low + c * step, step)], dst.at[pl.ds(c * step, step)], sems.at[n]
                )
                (moves[c] if at < nb else first).append(move)
                n += 1
        for move in first:
            move.start()
        for group in moves:
            for move in group:
                move.start()
        for move in first:
            move.wait()

        def ready(c):
            for move in moves[c]:
                move.wait()

        body(ready, *scalar_refs, *local_refs, *near_refs, *out_refs, *refs)

    rooms = [pltpu.VMEM((size,) + a.shape[1:], a.dtype) for a, _, size in far]
    count = nb * chunks + nm
    sems = [pltpu.SemaphoreType.DMA((count,))] if far else []
    return pl.pallas_call(
        kernel,
        in_specs=[SCALARS] * ns + [pl.BlockSpec(memory_space=pltpu.HBM)] * (nb + nm) + [FULL] * nn,
        out_specs=[FULL] * no,
        out_shape=[sds(*o) if final else (pltpu.HBM(o, F32) if n in away else in_vmem(o)) for n, o in enumerate(outs)],
        scratch_shapes=rooms + scratch + sems,
        compiler_params=pltpu.CompilerParams(vmem_limit_bytes=24 * 1024 * 1024),
    )(*scalars, *[pltpu.with_memory_space_constraint(a, pltpu.HBM) for a, _, _ in far], *near)


def room(*shape):
    return VMEM(shape, F32)


def turned(x, axis):
    def move(by):
        return lax.ppermute(x, axis, [(i, (i + by) % 4) for i in range(4)])

    return move(1), move(-1), move(2)


def shifted(x, by):
    pairs = [(i, i + by) for i in range(64) if 0 <= i + by < 64]
    return lax.ppermute(x, TM, pairs)


def local(
    state_map,
    input_map,
    closed_loop,
    feedback,
    value_matrix,
    gain_inverse,
    input_weight,
    state_weight,
    state_linear,
    input_linear,
    offset,
    upper_bound,
    states,
    inputs,
    multipliers,
    bound_mult,
    active,
):
    place = jnp.stack([lax.axis_index(a) for a in TM]).astype(jnp.int32)

    place, ahead = lax.optimization_barrier((place, multipliers[:8]))
    from_after = shifted(ahead, -1)
    (last,) = call(
        last_prediction_body, [],
        [(state_map, 15, 1), (input_map, 15, 1), (states, 8, 8), (inputs, 8, 8)], [], [],
        [(8, 256)], [],
    )
    from_before = shifted(last, 1)

    loops, last = lax.optimization_barrier((closed_loop, last))
    product, pairs, quads, half = call(
        block_product_body, [], [loops], [], [],
        [(256, 256), (4, 256, 256), (4, 256, 256), (256, 256)], [], chunks=4,
    )
    near = turned(product, "tm_2")

    defect, grad_input, sources, inner, costate, statistics = call(
        sources_body, [],
        [state_map, input_map, value_matrix, feedback, closed_loop],
        [states, inputs, multipliers, bound_mult, upper_bound, offset, state_weight, state_linear, input_linear, input_weight],
        [quads, half, from_before, from_after],
        [(16, 256), (16, 64), (16, 256), (16, 256), (8, 256), (8, 128)],
        [room(16, 256)], chunks=4,
    )
    costates = turned(costate, "tm_2")

    def join(axis, *parts):
        return call(
            functools.partial(join_body, axis=axis), [place], [], [],
            list(parts),
            [(4, 256, 256), (4, 8, 256), (264, 256)], [],
        )

    maps_z, vectors_z, group = join(2, product, *near, costate, *costates)
    near_x = turned(group, "tm_1")

    loops, group = lax.optimization_barrier((closed_loop, group))
    weight, third = call(
        weight_body, [], [loops, input_map, gain_inverse], [], [pairs, quads, half],
        [(256, 256), (256, 256)], [room(1024, 256), room(1024, 256)],
    )
    near_x, weight, third = lax.optimization_barrier((near_x, weight, third))

    maps_x, vectors_x, plane = join(1, group, *near_x)
    near_y = turned(plane, "tm_0")

    def sweep(loops, far, near, away):
        return call(
            sweep_body, [], [loops, input_map, gain_inverse], far, near,
            [(16, 256), (16, 64), (16, 64), (16, 256), (8, 256), (8, 256)], [room(16, 256)], away=away,
        )

    local_parts = [quads, inner, sources, grad_input, defect]
    loops, plane = lax.optimization_barrier((closed_loop, plane))
    local_state = sweep(loops, [], local_parts, range(5))[5]

    incoming, message = call(
        costate_body, [place], [], [],
        [plane, *near_y, maps_x, vectors_x, maps_z, vectors_z, weight, local_state, statistics],
        [(8, 256), (64, 1, 384)], [room(4, 256, 256), room(4, 8, 256)], away=(0, 1),
    )

    received = lax.all_to_all(message, TM, 0, 0, tiled=True)

    before, gain, base, push, entry, _ = sweep(
        closed_loop, local_parts + [incoming], [], range(6)
    )

    state_step, input_step, multiplier_step, bound_step, sums = call(
        functools.partial(finish_body, horizon=states.shape[0] * lax.axis_size(TM)), [place],
        [closed_loop, value_matrix, feedback],
        [active, upper_bound, inputs, input_weight, plane, *near_y, maps_x, maps_z, quads, half, third]
        + [entry, push, defect, before, gain, base],
        [received],
        [(16, 256), (16, 64), (16, 256), (16, 64), (1, 3)], [room(4, 256, 256)], final=True,
    )

    kkt_norms = sums.reshape(3)
    return (state_step, input_step, multiplier_step, bound_step, kkt_norms)


def solution(mesh):
    split = Mesh(
        mesh.devices.reshape(4, 4, 4, mesh.shape["batch"]), ("tm_0", "tm_1", "tm_2", "batch")
    )

    return jax.shard_map(
        local,
        mesh=split,
        in_specs=(P(BATCH_TM, None, None),) * 6 + (P("batch", None),) + (P(BATCH_TM, None),) * 10,
        out_specs=(P(BATCH_TM, None),) * 4 + (P("batch"),),
        check_vma=False,
    )
```

```python
import functools

import jax
import jax.numpy as jnp
from jax import lax
from jax.experimental import pallas as pl
from jax.experimental.pallas import tpu as pltpu
from jax.sharding import Mesh
from jax.sharding import PartitionSpec as P

TM = ("tm_0", "tm_1", "tm_2")
BATCH_TM = ("batch", "tm_0", "tm_1", "tm_2")
F32 = jnp.float32
BF16 = jnp.bfloat16
floor_share = 0.001
VMEM = pltpu.VMEM
SMEM = pltpu.SMEM


def halves(x):
    high = x.astype(BF16)
    low = (x - high.astype(F32)).astype(BF16)
    return high, low


def dot(a, b, ca, cb):
    return lax.dot_general(a, b, (((ca,), (cb,)), ((), ())), preferred_element_type=F32)


def mat_mul(a, b, ca=1, cb=0):
    ah, al = halves(a)
    bh, bl = halves(b)
    return dot(ah, bh, ca, cb) + (dot(ah, bl, ca, cb) + dot(al, bh, ca, cb))


def row_halves(v):
    high = v.astype(BF16).astype(F32)
    row = lax.broadcasted_iota(jnp.int32, (8, v.shape[1]), 0)
    both = jnp.where(row == 0, high, jnp.where(row == 1, v - high, 0.0))
    return both.astype(BF16)


def vec_mat(v, m, cb=0):
    lhs = row_halves(v)
    mh, ml = halves(m)
    r = dot(lhs, mh, 1, cb) + dot(lhs, ml, 1, cb)
    return jnp.sum(r, axis=0, keepdims=True)


def last_prediction_body(ready, f_ref, m_ref, x_ref, u_ref, out_ref):
    ready(0)
    v = vec_mat(x_ref[7:8, :], f_ref[0], 1) + vec_mat(u_ref[7:8, :], m_ref[0])
    out_ref[...] = jnp.broadcast_to(v, (8, 256))


def block_product_body(*refs, sections, rows):
    n = len(sections)
    far = refs[: n + rows]
    p_ref, pair_ref, quad_ref, half_ref = refs[n + rows: n + rows + 4]
    kept = refs[n + rows + 4: 2 * (n + rows) + 4]
    low_ref, sems = refs[2 * (n + rows) + 4:]
    a_ref = kept[0]
    loops = [
        pltpu.make_async_copy(far[0].at[pl.ds(4 * j, 4)], a_ref.at[pl.ds(4 * j, 4)], sems.at[j]) for j in range(4)
    ]
    rest = [pltpu.make_async_copy(f, k, sems.at[4 + i]) for i, (f, k) in enumerate(zip(far[1:], kept[1:]))]
    for move in loops + rest:
        move.start()
    for j in range(5):
        if j < 4:
            loops[j].wait()
            low_ref[j] = mat_mul(a_ref[4 * j + 1], a_ref[4 * j])
            pair_ref[j] = mat_mul(a_ref[4 * j + 3], a_ref[4 * j + 2])
        if j == 3:
            half_ref[...] = mat_mul(quad_ref[1], quad_ref[0])
        if j > 0:
            quad_ref[j - 1] = mat_mul(pair_ref[j - 1], low_ref[j - 1])
    p_ref[...] = mat_mul(mat_mul(quad_ref[3], quad_ref[2]), half_ref[...])
    for move in rest:
        move.wait()


def total(x):
    return jnp.sum(jnp.sum(x, axis=0, keepdims=True), axis=1, keepdims=True)


def sources_body(
    ready, f_ref, m_ref, v_ref, k_ref, a_ref,
    x_ref, u_ref, mult_ref, bm_ref, ub_ref, off_ref, sw_ref, sl_ref, il_ref, iw_ref,
    quad_ref, half_ref, p_ref, before_ref, next_ref,
    defect_ref, gi_ref, src_ref, b_ref, out_ref, stat_ref,
    gs_ref,
):
    gi_ref[...] = mat_mul(u_ref[...], iw_ref[...], 1, 1) + il_ref[...] + bm_ref[...]
    gs_ref[...] = sw_ref[...] * x_ref[...] + sl_ref[...] + mult_ref[...]
    src_ref[...] = x_ref[...] - off_ref[...]
    prev = before_ref[0:1, :]
    for i in range(4):
        for j in range(4):
            k = i * 4 + j
            follow = next_ref[0:1, :] if k == 15 else mult_ref[k + 1:k + 2, :]
            gs = gs_ref[k:k + 1, :] - vec_mat(follow, f_ref[k])
            gs_ref[k:k + 1, :] = gs
            gi = gi_ref[k:k + 1, :] - vec_mat(follow, m_ref[k], 1)
            gi_ref[k:k + 1, :] = gi
            d = src_ref[k:k + 1, :] - prev
            defect_ref[k:k + 1, :] = d
            src_ref[k:k + 1, :] = vec_mat(d, v_ref[k]) + gs + vec_mat(gi, k_ref[k])
            if k < 15:
                prev = vec_mat(x_ref[k:k + 1, :], f_ref[k], 1) + vec_mat(u_ref[k:k + 1, :], m_ref[k])
    b = [src_ref[4 * j + 3:4 * j + 4, :] for j in range(4)]
    for j in range(4):
        b_ref[4 * j + 3:4 * j + 4, :] = b[j]
    for m in (2, 1, 0):
        for j in range(4):
            k = 4 * j + m
            b[j] = vec_mat(b[j], a_ref[k]) + src_ref[k:k + 1, :]
            b_ref[k:k + 1, :] = b[j]
    upper = b[2] + vec_mat(b[3], quad_ref[2])
    c = b[0] + vec_mat(b[1], quad_ref[0]) + vec_mat(upper, half_ref[...])
    out_ref[0:256, :] = p_ref[...]
    out_ref[256:264, :] = jnp.broadcast_to(c, (8, 256))

    gap = bm_ref[...] * (ub_ref[...] - u_ref[...])
    d, gs, gi = defect_ref[...], gs_ref[...], gi_ref[...]
    off, sl, il, bm = off_ref[...], sl_ref[...], il_ref[...], bm_ref[...]
    found = (
        total(d * d),
        total(gs * gs) + total(gi * gi),
        total(gap * gap),
        total(off * off),
        total(sl * sl) + total(il * il),
        total(bm * bm),
    )
    lane = lax.broadcasted_iota(jnp.int32, (8, 128), 1)
    out = jnp.zeros((8, 128), F32)
    for n, s in enumerate(found):
        out = jnp.where(lane == n, s, out)
    stat_ref[...] = out


def weight_body(ready, a_ref, m_ref, g_ref, pair_ref, quad_ref, half_ref, w_ref, third_ref, b_ref, gb_ref):
    third_ref[...] = mat_mul(quad_ref[2], half_ref[...])
    for j in range(4):
        k = 4 * j
        r = 256 * j
        b_ref[r:r + 64, :] = mat_mul(m_ref[k], a_ref[k + 1], 1, 1)
        b_ref[r + 64:r + 128, :] = m_ref[k + 1]
        b_ref[r + 128:r + 192, :] = mat_mul(m_ref[k + 2], a_ref[k + 3], 1, 1)
        b_ref[r + 192:r + 256, :] = m_ref[k + 3]
        b_ref[r:r + 128, :] = mat_mul(b_ref[r:r + 128, :], pair_ref[j], 1, 1)
    for j in (1, 2, 3):
        b_ref[0:256 * j, :] = mat_mul(b_ref[0:256 * j, :], quad_ref[j], 1, 1)
    for k in range(16):
        gb_ref[64 * k:64 * k + 64, :] = mat_mul(g_ref[k], b_ref[64 * k:64 * k + 64, :])
    w_ref[...] = mat_mul(b_ref[...], gb_ref[...], 0, 0)


def backward_part(a_ref, m_ref, g_ref, quad_ref, b_ref, src_ref, gi_ref, lam, before_ref, gain_ref, base_ref, push_ref, after_ref, loaded=lambda: None):
    lams = [None, None, None, lam]
    for j in (2, 1, 0):
        known = b_ref[4 * j + 4:4 * j + 5, :]
        lams[j] = known if lams[j + 1] is None else vec_mat(lams[j + 1], quad_ref[j + 1]) + known
    before_ref[0:1, :] = vec_mat(lams[0], quad_ref[0]) + b_ref[0:1, :]
    for j in range(3):
        before_ref[4 * j + 4:4 * j + 5, :] = lams[j]
    loaded()
    for m in (3, 2, 1, 0):
        for j in range(4):
            k = 4 * j + m
            now = lams[j]
            after_ref[k:k + 1, :] = jnp.zeros((1, 256), F32) if now is None else now
            if m > 0:
                lams[j] = src_ref[k:k + 1, :] if now is None else vec_mat(now, a_ref[k]) + src_ref[k:k + 1, :]
                before_ref[k:k + 1, :] = lams[j]
    for k in range(16):
        base = gi_ref[k:k + 1, :] + vec_mat(after_ref[k:k + 1, :], m_ref[k], 1)
        base_ref[k:k + 1, :] = base
        gain = -vec_mat(base, g_ref[k])
        gain_ref[k:k + 1, :] = gain
        push_ref[k:k + 1, :] = vec_mat(gain, m_ref[k])


def local_ends(a_ref, push_ref, defect_ref):
    ends = [None] * 4
    for m in range(4):
        for j in range(4):
            k = 4 * j + m
            step = -defect_ref[k:k + 1, :] if m == 0 else ends[j] - defect_ref[k:k + 1, :]
            ends[j] = vec_mat(step, a_ref[k], 1) + push_ref[k:k + 1, :]
    return ends


def local_body(
    ready, a_ref, m_ref, g_ref, quad_ref, b_ref, src_ref, gi_ref, defect_ref,
    end_ref, before_ref, gain_ref, base_ref, push_ref, after_ref,
):
    backward_part(
        a_ref, m_ref, g_ref, quad_ref, b_ref, src_ref, gi_ref, None,
        before_ref, gain_ref, base_ref, push_ref, after_ref,
    )
    ends = local_ends(a_ref, push_ref, defect_ref)
    e = ends[0]
    for j in (1, 2, 3):
        e = vec_mat(e, quad_ref[j], 1) + ends[j]
    end_ref[...] = jnp.broadcast_to(e, (8, 256))


def order(ref, place, own, minus, plus, across):
    ref[place] = own
    ref[lax.rem(place + 1, 4)] = plus
    ref[lax.rem(place + 2, 4)] = across
    ref[lax.rem(place + 3, 4)] = minus


def join_body(ready, idx_ref, *refs, axis):
    place = idx_ref[axis]
    maps_ref, vectors_ref, out_ref = refs[-3:]
    parts = refs[:4]
    order(maps_ref, place, *[r[0:256, :] for r in parts])
    order(vectors_ref, place, *[r[256:264, :] for r in parts])
    high = mat_mul(maps_ref[3], maps_ref[2])
    low = mat_mul(maps_ref[1], maps_ref[0])
    v = vectors_ref[3, 0:1, :]
    for j in (2, 1, 0):
        v = vec_mat(v, maps_ref[j]) + vectors_ref[j, 0:1, :]
    out_ref[0:256, :] = mat_mul(high, low)
    out_ref[256:264, :] = jnp.broadcast_to(v, (8, 256))


def chain_back(maps, order, place):
    lam = order[3, 0:1, :]
    picked = jnp.where(place == 2, lam, 0.0)
    for j in (2, 1):
        lam = vec_mat(lam, maps[j]) + order[j, 0:1, :]
        picked = jnp.where(place == j - 1, lam, picked)
    return picked


def eye():
    r = lax.broadcasted_iota(jnp.int32, (256, 256), 0)
    c = lax.broadcasted_iota(jnp.int32, (256, 256), 1)
    return jnp.where(r == c, 1.0, 0.0).astype(F32)


def compose_body(ready, idx_ref, gx_ref, cx_ref, pz_ref, cz_ref, rest_z_ref, rest_ref, base_ref, until_z_ref, until_ref):
    x = idx_ref[1]
    z = idx_ref[2]

    def behind(maps, place):
        r = jnp.where(place < 3, maps[3], eye())
        r = jnp.where(place < 2, mat_mul(r, maps[2]), r)
        return jnp.where(place < 1, mat_mul(r, maps[1]), r)

    def ahead(maps, place):
        r = jnp.where(place > 0, maps[0], eye())
        r = jnp.where(place > 1, mat_mul(maps[1], r), r)
        return jnp.where(place > 2, mat_mul(maps[2], r), r)

    rest_z_ref[...] = behind(pz_ref, z)
    rest_ref[...] = mat_mul(behind(gx_ref, x), rest_z_ref[...])
    until_z_ref[...] = ahead(pz_ref, z)
    until_ref[...] = mat_mul(until_z_ref[...], ahead(gx_ref, x))
    lam = vec_mat(chain_back(gx_ref, cx_ref, x), rest_z_ref[...]) + chain_back(pz_ref, cz_ref, z)
    base_ref[...] = jnp.broadcast_to(lam, (8, 256))


def costate_body(
    ready, idx_ref, h0_ref, hm_ref, hp_ref, h2_ref,
    rest_z_ref, rest_ref, const_ref, w_ref, s0_ref, stat_ref,
    lam_ref, msg_ref, hy_ref, order_ref,
):
    y = idx_ref[0]
    x = idx_ref[1]
    refs = (h0_ref, hm_ref, hp_ref, h2_ref)
    order(hy_ref, y, *[r[0:256, :] for r in refs])
    order(order_ref, y, *[r[256:264, :] for r in refs])
    lam = vec_mat(chain_back(hy_ref, order_ref, y), rest_ref[...]) + const_ref[0:1, :]
    u1 = s0_ref[0:1, :] - vec_mat(lam, w_ref[...])
    u2 = vec_mat(u1, rest_z_ref[...], 1)
    u3 = vec_mat(u1, rest_ref[...], 1)
    d = lax.broadcasted_iota(jnp.int32, (64, 256), 0)
    group = lax.shift_right_logical(d, 2)
    plane = lax.shift_right_logical(d, 4)
    msg_ref[:, 0, 0:256] = jnp.where(group == y * 4 + x, u1, jnp.where(plane == y, u2, u3))
    msg_ref[:, 0, 256:384] = jnp.broadcast_to(stat_ref[0:1, :], (64, 128))
    lam_ref[...] = jnp.broadcast_to(lam, (8, 256))


def sweep_body(
    ready, quad_ref, a_ref, m_ref, g_ref, b_ref, src_ref, gi_ref, defect_ref, lam_ref,
    before_ref, gain_ref, base_ref, push_ref, entry_ref, after_ref,
):
    ready(0)
    backward_part(
        a_ref, m_ref, g_ref, quad_ref, b_ref, src_ref, gi_ref, lam_ref[0:1, :],
        before_ref, gain_ref, base_ref, push_ref, after_ref, lambda: ready(1),
    )
    ends = local_ends(a_ref, push_ref, defect_ref)
    entry_ref[...] = jnp.zeros_like(entry_ref)
    e = ends[0]
    for j in (1, 2, 3):
        entry_ref[j:j + 1, :] = e
        if j < 3:
            e = vec_mat(e, quad_ref[j], 1) + ends[j]


def chain_forth(maps, sums, place):
    e = sums[0]
    picked = jnp.where(place == 1, e, 0.0)
    for j in (1, 2):
        e = vec_mat(e, maps(j), 1) + sums[j]
        picked = jnp.where(place == j + 1, e, picked)
    return picked


def finish_body(
    ready, idx_ref,
    h0_ref, hm_ref, hp_ref, h2_ref, gx_ref, pz_ref, until_z_ref, until_ref, quad_ref, half_ref, third_ref,
    a_ref, v_ref, k_ref,
    active_ref, ub_ref, u_ref, iw_ref, defect_ref, before_ref, gain_ref, base_ref, push_ref, entry_ref,
    msg_ref,
    ss_ref, is_ref, ms_ref, bs_ref, norm_ref,
    hy_ref,
    *, horizon,
):
    y = idx_ref[0]
    x = idx_ref[1]
    z = idx_ref[2]
    d = lax.broadcasted_iota(jnp.int32, (64, 256), 0)
    plane = lax.shift_right_logical(d, 4)
    group = lax.shift_right_logical(d, 2)
    msg = msg_ref[:, 0, 0:256]

    def picked(mask):
        return jnp.sum(jnp.where(mask, msg, 0.0), axis=0, keepdims=True)

    ready(0)
    order(hy_ref, y, *[r[0:256, :] for r in (h0_ref, hm_ref, hp_ref, h2_ref)])
    ey = chain_forth(lambda j: hy_ref[j], [picked(plane == j) for j in range(3)], y)
    ex = chain_forth(lambda j: gx_ref[j - 1], [picked(group == y * 4 + j) for j in range(3)], x)
    ez = chain_forth(lambda j: pz_ref[j - 1], [picked(d == y * 16 + x * 4 + j) for j in range(3)], z)
    e = vec_mat(ey, until_ref[...], 1) + vec_mat(ex, until_z_ref[...], 1) + ez
    sums = jnp.sum(msg_ref[:, 0, 256:384], axis=0, keepdims=True)
    lane = lax.broadcasted_iota(jnp.int32, (1, 128), 1)
    share = floor_share * horizon
    floors = jnp.where(lane == 0, share * 256, jnp.where(lane == 1, share * 320, share * 64))
    norm_ref[...] = jnp.sqrt(sums / (pltpu.roll(sums, 125, 1) + floors))[:, 0:3]

    entries = [e] + [
        vec_mat(e, m, 1) + entry_ref[j:j + 1, :]
        for j, m in ((1, quad_ref[0]), (2, half_ref[...]), (3, third_ref[...]))
    ]
    ready(1)
    for m in range(4):
        for j in range(4):
            k = 4 * j + m
            step = entries[j] - defect_ref[k:k + 1, :]
            ss_ref[k:k + 1, :] = step
            if m < 3:
                entries[j] = vec_mat(step, a_ref[k], 1) + push_ref[k:k + 1, :]
    ready(2)
    for k in range(16):
        step = ss_ref[k:k + 1, :]
        ms_ref[k:k + 1, :] = vec_mat(step - defect_ref[k:k + 1, :], v_ref[k]) + before_ref[k:k + 1, :]
        is_ref[k:k + 1, :] = vec_mat(step, k_ref[k], 1) + gain_ref[k:k + 1, :]
    chosen = active_ref[...].astype(F32)
    step = (1.0 - chosen) * is_ref[...] + chosen * (ub_ref[...] - u_ref[...])
    is_ref[...] = step
    bs_ref[...] = chosen * (base_ref[...] + mat_mul(step, iw_ref[...], 1, 1))


def sds(*shape):
    return jax.ShapeDtypeStruct(shape, F32)


SCALARS = pl.BlockSpec(memory_space=SMEM)
FULL = pl.BlockSpec(memory_space=VMEM)


def in_vmem(shape):
    return pltpu.VMEM(shape, F32)


def part(array, slot=0, chunks=1, low=0, size=None):
    return array, slot, chunks, low, array.shape[0] if size is None else size


def call(body, scalars, big, small, near, outs, scratch, final=False, away=()):
    ns, nn, no = len(scalars), len(near), len(outs)
    far = list(big) + [part(a, -1) for a in small]
    slots = max([p[1] + p[2] for p in far] + [0])

    def kernel(*refs):
        refs = list(refs)

        def take(n):
            out = refs[:n]
            del refs[:n]
            return out

        scalar_refs, far_refs, near_refs, out_refs, local_refs = take(ns), take(len(far)), take(nn), take(no), take(len(far))
        sems = refs.pop() if far else None
        moves = [[] for _ in range(slots)]
        first = []
        n = 0
        for (_, slot, chunks, low, size), src, dst in zip(far, far_refs, local_refs):
            step = size // chunks
            for c in range(chunks):
                move = pltpu.make_async_copy(
                    src.at[pl.ds(low + c * step, step)], dst.at[pl.ds(c * step, step)], sems.at[n]
                )
                (first if slot < 0 else moves[slot + c]).append(move)
                n += 1
        for group in [first] + moves:
            for move in group:
                move.start()
        for move in first:
            move.wait()

        def ready(c):
            for move in moves[c]:
                move.wait()

        body(ready, *scalar_refs, *local_refs, *near_refs, *out_refs, *refs)

    rooms = [pltpu.VMEM((p[4],) + p[0].shape[1:], p[0].dtype) for p in far]
    sems = [pltpu.SemaphoreType.DMA((sum(p[2] for p in far),))] if far else []
    return pl.pallas_call(
        kernel,
        in_specs=[SCALARS] * ns + [pl.BlockSpec(memory_space=pltpu.HBM)] * len(far) + [FULL] * nn,
        out_specs=[FULL] * no,
        out_shape=[sds(*o) if final else (pltpu.HBM(o, F32) if n in away else in_vmem(o)) for n, o in enumerate(outs)],
        scratch_shapes=rooms + scratch + sems,
        compiler_params=pltpu.CompilerParams(vmem_limit_bytes=24 * 1024 * 1024),
    )(*scalars, *[pltpu.with_memory_space_constraint(p[0], pltpu.HBM) for p in far], *near)


def room(*shape):
    return VMEM(shape, F32)


def turned(x, axis):
    def move(by):
        return lax.ppermute(x, axis, [(i, (i + by) % 4) for i in range(4)])

    return move(1), move(-1), move(2)


def shifted(x, by):
    pairs = [(i, i + by) for i in range(64) if 0 <= i + by < 64]
    return lax.ppermute(x, TM, pairs)


def local(
    state_map,
    input_map,
    closed_loop,
    feedback,
    value_matrix,
    gain_inverse,
    input_weight,
    state_weight,
    state_linear,
    input_linear,
    offset,
    upper_bound,
    states,
    inputs,
    multipliers,
    bound_mult,
    active,
):
    place = jnp.stack([lax.axis_index(a) for a in TM]).astype(jnp.int32)

    place, ahead = lax.optimization_barrier((place, multipliers[:8]))
    from_after = shifted(ahead, -1)
    (last,) = call(
        last_prediction_body, [],
        [part(state_map, 0, 1, 15, 1), part(input_map, 0, 1, 15, 1), part(states, 0, 1, 8, 8), part(inputs, 0, 1, 8, 8)],
        [], [], [(8, 256)], [],
    )
    from_before = shifted(last, 1)

    loops, last = lax.optimization_barrier((closed_loop, last))
    sections = [loops, state_map, input_map, value_matrix, feedback, gain_inverse]
    rows = [
        states, inputs, multipliers, bound_mult, upper_bound, offset, state_weight, state_linear, input_linear,
        input_weight,
    ]
    kept = sections + rows
    out = pl.pallas_call(
        functools.partial(block_product_body, sections=sections, rows=len(rows)),
        in_specs=[pl.BlockSpec(memory_space=pltpu.HBM)] * len(kept),
        out_specs=[FULL] * (4 + len(kept)),
        out_shape=[in_vmem(o) for o in [(256, 256), (4, 256, 256), (4, 256, 256), (256, 256)] + [k.shape for k in kept]],
        scratch_shapes=[room(4, 256, 256), pltpu.SemaphoreType.DMA((3 + len(kept),))],
        compiler_params=pltpu.CompilerParams(vmem_limit_bytes=24 * 1024 * 1024),
        name="block_product",
    )(*[pltpu.with_memory_space_constraint(k, pltpu.HBM) for k in kept])
    product, pairs, quads, half = out[:4]
    loop_v, map_v, push_v, value_v, feed_v, inverse_v = out[4:10]
    rows_v = out[10:]

    defect, grad_input, sources, inner, block, statistics = call(
        sources_body, [],
        [], [],
        [map_v, push_v, value_v, feed_v, loop_v, *rows_v, quads, half, product, from_before, from_after],
        [(16, 256), (16, 64), (16, 256), (16, 256), (264, 256), (8, 128)],
        [room(16, 256)],
    )
    near_z = turned(block, "tm_2")

    def join(axis, *parts):
        return call(
            functools.partial(join_body, axis=axis), [place], [], [],
            list(parts),
            [(4, 256, 256), (4, 8, 256), (264, 256)], [],
        )

    pairs, block = lax.optimization_barrier((pairs, block))
    weight, third = call(
        weight_body, [], [], [], [loop_v, push_v, inverse_v, pairs, quads, half],
        [(256, 256), (256, 256)], [room(1024, 256), room(1024, 256)],
    )
    near_z, weight, third = lax.optimization_barrier((near_z, weight, third))
    maps_z, vectors_z, group = join(2, block, *near_z)
    near_x = turned(group, "tm_1")

    inner, group = lax.optimization_barrier((inner, group))
    (local_state,) = call(
        local_body, [], [], [],
        [loop_v, push_v, inverse_v, quads, inner, sources, grad_input, defect],
        [(8, 256)],
        [room(16, 256), room(16, 64), room(16, 64), room(16, 256), room(16, 256)],
    )
    near_x, local_state = lax.optimization_barrier((near_x, local_state))
    maps_x, vectors_x, plane = join(1, group, *near_x)
    near_y = turned(plane, "tm_0")

    maps_x, plane = lax.optimization_barrier((maps_x, plane))
    rest_z, rest, constant, until_z, until = call(
        compose_body, [place], [], [], [maps_x, vectors_x, maps_z, vectors_z],
        [(256, 256), (256, 256), (8, 256), (256, 256), (256, 256)], [],
    )

    incoming, message = call(
        costate_body, [place], [], [],
        [plane, *near_y, rest_z, rest, constant, weight, local_state, statistics],
        [(8, 256), (64, 1, 384)], [room(4, 256, 256), room(4, 8, 256)], away=(0, 1),
    )

    received = lax.all_to_all(message, TM, 0, 0, tiled=True)

    before, gain, base, push, entry = call(
        sweep_body, [], [part(quads), part(closed_loop, 1), part(input_map, 1), part(gain_inverse, 1)],
        [inner, sources, grad_input, defect, incoming], [],
        [(16, 256), (16, 64), (16, 64), (16, 256), (8, 256)], [room(16, 256)], away=range(5),
    )

    state_step, input_step, multiplier_step, bound_step, sums = call(
        functools.partial(finish_body, horizon=states.shape[0] * lax.axis_size(TM)), [place],
        [part(a) for a in (plane, *near_y)]
        + [part(a, 0, 1, 1, 2) for a in (maps_x, maps_z)]
        + [part(until_z), part(until), part(quads, 0, 1, 0, 1), part(half), part(third)]
        + [part(closed_loop, 1), part(value_matrix, 2), part(feedback, 2)],
        [active, upper_bound, inputs, input_weight, defect, before, gain, base, push, entry],
        [received],
        [(16, 256), (16, 64), (16, 256), (16, 64), (1, 3)],
        [room(4, 256, 256)], final=True,
    )

    kkt_norms = sums.reshape(3)
    return (state_step, input_step, multiplier_step, bound_step, kkt_norms)


def solution(mesh):
    split = Mesh(
        mesh.devices.reshape(4, 4, 4, mesh.shape["batch"]), ("tm_0", "tm_1", "tm_2", "batch")
    )

    return jax.shard_map(
        local,
        mesh=split,
        in_specs=(P(BATCH_TM, None, None),) * 6 + (P("batch", None),) + (P(BATCH_TM, None),) * 10,
        out_specs=(P(BATCH_TM, None),) * 4 + (P("batch"),),
        check_vma=False,
    )
```

```python
import functools

import jax
import jax.numpy as jnp
from jax import lax
from jax.experimental import pallas as pl
from jax.experimental.pallas import tpu as pltpu
from jax.sharding import Mesh
from jax.sharding import PartitionSpec as P

TM = ("tm_0", "tm_1", "tm_2")
BATCH_TM = ("batch", "tm_0", "tm_1", "tm_2")
F32 = jnp.float32
BF16 = jnp.bfloat16
floor_share = 0.001
VMEM = pltpu.VMEM
SMEM = pltpu.SMEM


def halves(x):
    high = x.astype(BF16)
    low = (x - high.astype(F32)).astype(BF16)
    return high, low


def dot(a, b, ca, cb):
    return lax.dot_general(a, b, (((ca,), (cb,)), ((), ())), preferred_element_type=F32)


def mat_mul(a, b, ca=1, cb=0):
    ah, al = halves(a)
    bh, bl = halves(b)
    return dot(ah, bh, ca, cb) + (dot(ah, bl, ca, cb) + dot(al, bh, ca, cb))


def row_halves(v):
    high = v.astype(BF16).astype(F32)
    row = lax.broadcasted_iota(jnp.int32, (8, v.shape[1]), 0)
    both = jnp.where(row == 0, high, jnp.where(row == 1, v - high, 0.0))
    return both.astype(BF16)


def vec_mat(v, m, cb=0):
    lhs = row_halves(v)
    mh, ml = halves(m)
    r = dot(lhs, mh, 1, cb) + dot(lhs, ml, 1, cb)
    return jnp.sum(r, axis=0, keepdims=True)


def last_prediction_body(ready, f_ref, m_ref, x_ref, u_ref, out_ref):
    ready(0)
    v = vec_mat(x_ref[7:8, :], f_ref[0], 1) + vec_mat(u_ref[7:8, :], m_ref[0])
    out_ref[...] = jnp.broadcast_to(v, (8, 256))


def block_product_body(*refs, sections, rows):
    n = len(sections)
    far = refs[: n + rows]
    p_ref, pair_ref, quad_ref, half_ref = refs[n + rows: n + rows + 4]
    kept = refs[n + rows + 4: 2 * (n + rows) + 4]
    low_ref, sems = refs[2 * (n + rows) + 4:]
    a_ref = kept[0]
    loops = [
        pltpu.make_async_copy(far[0].at[pl.ds(4 * j, 4)], a_ref.at[pl.ds(4 * j, 4)], sems.at[j]) for j in range(4)
    ]
    rest = [pltpu.make_async_copy(f, k, sems.at[4 + i]) for i, (f, k) in enumerate(zip(far[1:], kept[1:]))]
    for move in loops + rest:
        move.start()
    for j in range(5):
        if j < 4:
            loops[j].wait()
            low_ref[j] = mat_mul(a_ref[4 * j + 1], a_ref[4 * j])
            pair_ref[j] = mat_mul(a_ref[4 * j + 3], a_ref[4 * j + 2])
        if j == 3:
            half_ref[...] = mat_mul(quad_ref[1], quad_ref[0])
        if j > 0:
            quad_ref[j - 1] = mat_mul(pair_ref[j - 1], low_ref[j - 1])
    p_ref[...] = mat_mul(mat_mul(quad_ref[3], quad_ref[2]), half_ref[...])
    for move in rest:
        move.wait()


def total(x):
    return jnp.sum(jnp.sum(x, axis=0, keepdims=True), axis=1, keepdims=True)


def sources_body(
    ready, f_ref, m_ref, v_ref, k_ref, a_ref,
    x_ref, u_ref, mult_ref, bm_ref, ub_ref, off_ref, sw_ref, sl_ref, il_ref, iw_ref,
    quad_ref, half_ref, p_ref, before_ref, next_ref,
    defect_ref, gi_ref, src_ref, b_ref, out_ref, stat_ref,
    gs_ref,
):
    gi_ref[...] = mat_mul(u_ref[...], iw_ref[...], 1, 1) + il_ref[...] + bm_ref[...]
    gs_ref[...] = sw_ref[...] * x_ref[...] + sl_ref[...] + mult_ref[...]
    src_ref[...] = x_ref[...] - off_ref[...]
    prev = before_ref[0:1, :]
    for i in range(4):
        for j in range(4):
            k = i * 4 + j
            follow = next_ref[0:1, :] if k == 15 else mult_ref[k + 1:k + 2, :]
            gs = gs_ref[k:k + 1, :] - vec_mat(follow, f_ref[k])
            gs_ref[k:k + 1, :] = gs
            gi = gi_ref[k:k + 1, :] - vec_mat(follow, m_ref[k], 1)
            gi_ref[k:k + 1, :] = gi
            d = src_ref[k:k + 1, :] - prev
            defect_ref[k:k + 1, :] = d
            src_ref[k:k + 1, :] = vec_mat(d, v_ref[k]) + gs + vec_mat(gi, k_ref[k])
            if k < 15:
                prev = vec_mat(x_ref[k:k + 1, :], f_ref[k], 1) + vec_mat(u_ref[k:k + 1, :], m_ref[k])
    b = [src_ref[4 * j + 3:4 * j + 4, :] for j in range(4)]
    for j in range(4):
        b_ref[4 * j + 3:4 * j + 4, :] = b[j]
    for m in (2, 1, 0):
        for j in range(4):
            k = 4 * j + m
            b[j] = vec_mat(b[j], a_ref[k]) + src_ref[k:k + 1, :]
            b_ref[k:k + 1, :] = b[j]
    upper = b[2] + vec_mat(b[3], quad_ref[2])
    c = b[0] + vec_mat(b[1], quad_ref[0]) + vec_mat(upper, half_ref[...])
    out_ref[0:256, :] = p_ref[...]
    out_ref[256:264, :] = jnp.broadcast_to(c, (8, 256))

    gap = bm_ref[...] * (ub_ref[...] - u_ref[...])
    d, gs, gi = defect_ref[...], gs_ref[...], gi_ref[...]
    off, sl, il, bm = off_ref[...], sl_ref[...], il_ref[...], bm_ref[...]
    found = (
        total(d * d),
        total(gs * gs) + total(gi * gi),
        total(gap * gap),
        total(off * off),
        total(sl * sl) + total(il * il),
        total(bm * bm),
    )
    lane = lax.broadcasted_iota(jnp.int32, (8, 128), 1)
    out = jnp.zeros((8, 128), F32)
    for n, s in enumerate(found):
        out = jnp.where(lane == n, s, out)
    stat_ref[...] = out


def weight_body(ready, a_ref, m_ref, g_ref, pair_ref, quad_ref, half_ref, w_ref, third_ref, b_ref, gb_ref):
    third_ref[...] = mat_mul(quad_ref[2], half_ref[...])
    for j in range(4):
        k = 4 * j
        r = 256 * j
        b_ref[r:r + 64, :] = mat_mul(m_ref[k], a_ref[k + 1], 1, 1)
        b_ref[r + 64:r + 128, :] = m_ref[k + 1]
        b_ref[r + 128:r + 192, :] = mat_mul(m_ref[k + 2], a_ref[k + 3], 1, 1)
        b_ref[r + 192:r + 256, :] = m_ref[k + 3]
        b_ref[r:r + 128, :] = mat_mul(b_ref[r:r + 128, :], pair_ref[j], 1, 1)
    for j in (1, 2, 3):
        b_ref[0:256 * j, :] = mat_mul(b_ref[0:256 * j, :], quad_ref[j], 1, 1)
    for k in range(16):
        gb_ref[64 * k:64 * k + 64, :] = mat_mul(g_ref[k], b_ref[64 * k:64 * k + 64, :])
    w_ref[...] = mat_mul(b_ref[...], gb_ref[...], 0, 0)


def backward_part(a_ref, m_ref, g_ref, quad_ref, b_ref, src_ref, gi_ref, lam, before_ref, gain_ref, base_ref, push_ref, after_ref, loaded=lambda: None):
    lams = [None, None, None, lam]
    for j in (2, 1, 0):
        known = b_ref[4 * j + 4:4 * j + 5, :]
        lams[j] = known if lams[j + 1] is None else vec_mat(lams[j + 1], quad_ref[j + 1]) + known
    before_ref[0:1, :] = vec_mat(lams[0], quad_ref[0]) + b_ref[0:1, :]
    for j in range(3):
        before_ref[4 * j + 4:4 * j + 5, :] = lams[j]
    loaded()
    for m in (3, 2, 1, 0):
        for j in range(4):
            k = 4 * j + m
            now = lams[j]
            after_ref[k:k + 1, :] = jnp.zeros((1, 256), F32) if now is None else now
            if m > 0:
                lams[j] = src_ref[k:k + 1, :] if now is None else vec_mat(now, a_ref[k]) + src_ref[k:k + 1, :]
                before_ref[k:k + 1, :] = lams[j]
    for k in range(16):
        base = gi_ref[k:k + 1, :] + vec_mat(after_ref[k:k + 1, :], m_ref[k], 1)
        base_ref[k:k + 1, :] = base
        gain = -vec_mat(base, g_ref[k])
        gain_ref[k:k + 1, :] = gain
        push_ref[k:k + 1, :] = vec_mat(gain, m_ref[k])


def local_ends(a_ref, push_ref, defect_ref):
    ends = [None] * 4
    for m in range(4):
        for j in range(4):
            k = 4 * j + m
            step = -defect_ref[k:k + 1, :] if m == 0 else ends[j] - defect_ref[k:k + 1, :]
            ends[j] = vec_mat(step, a_ref[k], 1) + push_ref[k:k + 1, :]
    return ends


def local_body(
    ready, a_ref, m_ref, g_ref, quad_ref, b_ref, src_ref, gi_ref, defect_ref,
    end_ref, before_ref, gain_ref, base_ref, push_ref, after_ref,
):
    backward_part(
        a_ref, m_ref, g_ref, quad_ref, b_ref, src_ref, gi_ref, None,
        before_ref, gain_ref, base_ref, push_ref, after_ref,
    )
    ends = local_ends(a_ref, push_ref, defect_ref)
    e = ends[0]
    for j in (1, 2, 3):
        e = vec_mat(e, quad_ref[j], 1) + ends[j]
    end_ref[...] = jnp.broadcast_to(e, (8, 256))


def order(ref, place, own, minus, plus, across):
    ref[place] = own
    ref[lax.rem(place + 1, 4)] = plus
    ref[lax.rem(place + 2, 4)] = across
    ref[lax.rem(place + 3, 4)] = minus


def join_body(ready, idx_ref, *refs, axis):
    place = idx_ref[axis]
    maps_ref, vectors_ref, out_ref = refs[-3:]
    parts = refs[:4]
    order(maps_ref, place, *[r[0:256, :] for r in parts])
    order(vectors_ref, place, *[r[256:264, :] for r in parts])
    high = mat_mul(maps_ref[3], maps_ref[2])
    low = mat_mul(maps_ref[1], maps_ref[0])
    v = vectors_ref[3, 0:1, :]
    for j in (2, 1, 0):
        v = vec_mat(v, maps_ref[j]) + vectors_ref[j, 0:1, :]
    out_ref[0:256, :] = mat_mul(high, low)
    out_ref[256:264, :] = jnp.broadcast_to(v, (8, 256))


def chain_back(maps, order, place):
    lam = order[3, 0:1, :]
    picked = jnp.where(place == 2, lam, 0.0)
    for j in (2, 1):
        lam = vec_mat(lam, maps[j]) + order[j, 0:1, :]
        picked = jnp.where(place == j - 1, lam, picked)
    return picked


def eye():
    r = lax.broadcasted_iota(jnp.int32, (256, 256), 0)
    c = lax.broadcasted_iota(jnp.int32, (256, 256), 1)
    return jnp.where(r == c, 1.0, 0.0).astype(F32)


def compose_body(ready, idx_ref, gx_ref, cx_ref, pz_ref, cz_ref, rest_z_ref, rest_ref, base_ref, until_z_ref, until_ref):
    x = idx_ref[1]
    z = idx_ref[2]

    def behind(maps, place):
        r = jnp.where(place < 3, maps[3], eye())
        r = jnp.where(place < 2, mat_mul(r, maps[2]), r)
        return jnp.where(place < 1, mat_mul(r, maps[1]), r)

    def ahead(maps, place):
        r = jnp.where(place > 0, maps[0], eye())
        r = jnp.where(place > 1, mat_mul(maps[1], r), r)
        return jnp.where(place > 2, mat_mul(maps[2], r), r)

    rest_z_ref[...] = behind(pz_ref, z)
    rest_ref[...] = mat_mul(behind(gx_ref, x), rest_z_ref[...])
    until_z_ref[...] = ahead(pz_ref, z)
    until_ref[...] = mat_mul(until_z_ref[...], ahead(gx_ref, x))
    lam = vec_mat(chain_back(gx_ref, cx_ref, x), rest_z_ref[...]) + chain_back(pz_ref, cz_ref, z)
    base_ref[...] = jnp.broadcast_to(lam, (8, 256))


def costate_body(
    ready, idx_ref, h0_ref, hm_ref, hp_ref, h2_ref,
    rest_z_ref, rest_ref, const_ref, w_ref, s0_ref, stat_ref,
    lam_ref, msg_ref, hy_ref, order_ref,
):
    y = idx_ref[0]
    x = idx_ref[1]
    refs = (h0_ref, hm_ref, hp_ref, h2_ref)
    order(hy_ref, y, *[r[0:256, :] for r in refs])
    order(order_ref, y, *[r[256:264, :] for r in refs])
    lam = vec_mat(chain_back(hy_ref, order_ref, y), rest_ref[...]) + const_ref[0:1, :]
    u1 = s0_ref[0:1, :] - vec_mat(lam, w_ref[...])
    u2 = vec_mat(u1, rest_z_ref[...], 1)
    u3 = vec_mat(u1, rest_ref[...], 1)
    d = lax.broadcasted_iota(jnp.int32, (64, 256), 0)
    group = lax.shift_right_logical(d, 2)
    plane = lax.shift_right_logical(d, 4)
    msg_ref[:, 0, 0:256] = jnp.where(group == y * 4 + x, u1, jnp.where(plane == y, u2, u3))
    msg_ref[:, 0, 256:384] = jnp.broadcast_to(stat_ref[0:1, :], (64, 128))
    lam_ref[...] = jnp.broadcast_to(lam, (8, 256))


def sweep_body(
    ready, quad_ref, a_ref, m_ref, g_ref, b_ref, src_ref, gi_ref, defect_ref, lam_ref,
    before_ref, gain_ref, base_ref, push_ref, entry_ref, after_ref,
):
    ready(0)
    backward_part(
        a_ref, m_ref, g_ref, quad_ref, b_ref, src_ref, gi_ref, lam_ref[0:1, :],
        before_ref, gain_ref, base_ref, push_ref, after_ref, lambda: ready(1),
    )
    ends = local_ends(a_ref, push_ref, defect_ref)
    entry_ref[...] = jnp.zeros_like(entry_ref)
    e = ends[0]
    for j in (1, 2, 3):
        entry_ref[j:j + 1, :] = e
        if j < 3:
            e = vec_mat(e, quad_ref[j], 1) + ends[j]


def chain_forth(maps, sums, place):
    e = sums[0]
    picked = jnp.where(place == 1, e, 0.0)
    for j in (1, 2):
        e = vec_mat(e, maps(j), 1) + sums[j]
        picked = jnp.where(place == j + 1, e, picked)
    return picked


def finish_body(
    ready, idx_ref,
    h0_ref, hm_ref, hp_ref, h2_ref, gx_ref, pz_ref, until_z_ref, until_ref, quad_ref, half_ref, third_ref,
    a_ref, v_ref, k_ref,
    active_ref, ub_ref, u_ref, iw_ref, defect_ref, before_ref, gain_ref, base_ref, push_ref, entry_ref,
    msg_ref,
    ss_ref, is_ref, ms_ref, bs_ref, norm_ref,
    hy_ref,
    *, horizon,
):
    y = idx_ref[0]
    x = idx_ref[1]
    z = idx_ref[2]
    d = lax.broadcasted_iota(jnp.int32, (64, 256), 0)
    plane = lax.shift_right_logical(d, 4)
    group = lax.shift_right_logical(d, 2)
    msg = msg_ref[:, 0, 0:256]

    def picked(mask):
        return jnp.sum(jnp.where(mask, msg, 0.0), axis=0, keepdims=True)

    ready(0)
    order(hy_ref, y, *[r[0:256, :] for r in (h0_ref, hm_ref, hp_ref, h2_ref)])
    ey = chain_forth(lambda j: hy_ref[j], [picked(plane == j) for j in range(3)], y)
    ex = chain_forth(lambda j: gx_ref[j - 1], [picked(group == y * 4 + j) for j in range(3)], x)
    ez = chain_forth(lambda j: pz_ref[j - 1], [picked(d == y * 16 + x * 4 + j) for j in range(3)], z)
    e = vec_mat(ey, until_ref[...], 1) + vec_mat(ex, until_z_ref[...], 1) + ez
    sums = jnp.sum(msg_ref[:, 0, 256:384], axis=0, keepdims=True)
    lane = lax.broadcasted_iota(jnp.int32, (1, 128), 1)
    share = floor_share * horizon
    floors = jnp.where(lane == 0, share * 256, jnp.where(lane == 1, share * 320, share * 64))
    norm_ref[...] = jnp.sqrt(sums / (pltpu.roll(sums, 125, 1) + floors))[:, 0:3]

    entries = [e] + [
        vec_mat(e, m, 1) + entry_ref[j:j + 1, :]
        for j, m in ((1, quad_ref[0]), (2, half_ref[...]), (3, third_ref[...]))
    ]
    ready(1)
    ready(2)
    for m in range(4):
        steps = [None] * 4
        for j in range(4):
            k = 4 * j + m
            step = entries[j] - defect_ref[k:k + 1, :]
            steps[j] = step
            ss_ref[k:k + 1, :] = step
            if m < 3:
                entries[j] = vec_mat(step, a_ref[k], 1) + push_ref[k:k + 1, :]
        for j in range(4):
            k = 4 * j + m
            step = steps[j]
            ms_ref[k:k + 1, :] = vec_mat(step - defect_ref[k:k + 1, :], v_ref[k]) + before_ref[k:k + 1, :]
            is_ref[k:k + 1, :] = vec_mat(step, k_ref[k], 1) + gain_ref[k:k + 1, :]
    chosen = active_ref[...].astype(F32)
    step = (1.0 - chosen) * is_ref[...] + chosen * (ub_ref[...] - u_ref[...])
    is_ref[...] = step
    bs_ref[...] = chosen * (base_ref[...] + mat_mul(step, iw_ref[...], 1, 1))


def sds(*shape):
    return jax.ShapeDtypeStruct(shape, F32)


SCALARS = pl.BlockSpec(memory_space=SMEM)
FULL = pl.BlockSpec(memory_space=VMEM)


def in_vmem(shape):
    return pltpu.VMEM(shape, F32)


def part(array, slot=0, chunks=1, low=0, size=None):
    return array, slot, chunks, low, array.shape[0] if size is None else size


def call(body, scalars, big, small, near, outs, scratch, final=False, away=()):
    ns, nn, no = len(scalars), len(near), len(outs)
    far = list(big) + [part(a, -1) for a in small]
    slots = max([p[1] + p[2] for p in far] + [0])

    def kernel(*refs):
        refs = list(refs)

        def take(n):
            out = refs[:n]
            del refs[:n]
            return out

        scalar_refs, far_refs, near_refs, out_refs, local_refs = take(ns), take(len(far)), take(nn), take(no), take(len(far))
        sems = refs.pop() if far else None
        moves = [[] for _ in range(slots)]
        first = []
        n = 0
        for (_, slot, chunks, low, size), src, dst in zip(far, far_refs, local_refs):
            step = size // chunks
            for c in range(chunks):
                move = pltpu.make_async_copy(
                    src.at[pl.ds(low + c * step, step)], dst.at[pl.ds(c * step, step)], sems.at[n]
                )
                (first if slot < 0 else moves[slot + c]).append(move)
                n += 1
        for group in [first] + moves:
            for move in group:
                move.start()
        for move in first:
            move.wait()

        def ready(c):
            for move in moves[c]:
                move.wait()

        body(ready, *scalar_refs, *local_refs, *near_refs, *out_refs, *refs)

    rooms = [pltpu.VMEM((p[4],) + p[0].shape[1:], p[0].dtype) for p in far]
    sems = [pltpu.SemaphoreType.DMA((sum(p[2] for p in far),))] if far else []
    return pl.pallas_call(
        kernel,
        in_specs=[SCALARS] * ns + [pl.BlockSpec(memory_space=pltpu.HBM)] * len(far) + [FULL] * nn,
        out_specs=[FULL] * no,
        out_shape=[sds(*o) if final else (pltpu.HBM(o, F32) if n in away else in_vmem(o)) for n, o in enumerate(outs)],
        scratch_shapes=rooms + scratch + sems,
        compiler_params=pltpu.CompilerParams(vmem_limit_bytes=24 * 1024 * 1024),
    )(*scalars, *[pltpu.with_memory_space_constraint(p[0], pltpu.HBM) for p in far], *near)


def room(*shape):
    return VMEM(shape, F32)


def turned(x, axis):
    def move(by):
        return lax.ppermute(x, axis, [(i, (i + by) % 4) for i in range(4)])

    return move(1), move(-1), move(2)


def shifted(x, by):
    pairs = [(i, i + by) for i in range(64) if 0 <= i + by < 64]
    return lax.ppermute(x, TM, pairs)


def local(
    state_map,
    input_map,
    closed_loop,
    feedback,
    value_matrix,
    gain_inverse,
    input_weight,
    state_weight,
    state_linear,
    input_linear,
    offset,
    upper_bound,
    states,
    inputs,
    multipliers,
    bound_mult,
    active,
):
    place = jnp.stack([lax.axis_index(a) for a in TM]).astype(jnp.int32)

    place, ahead = lax.optimization_barrier((place, multipliers[:8]))
    from_after = shifted(ahead, -1)
    (last,) = call(
        last_prediction_body, [],
        [part(state_map, 0, 1, 15, 1), part(input_map, 0, 1, 15, 1), part(states, 0, 1, 8, 8), part(inputs, 0, 1, 8, 8)],
        [], [], [(8, 256)], [],
    )
    from_before = shifted(last, 1)

    loops, last = lax.optimization_barrier((closed_loop, last))
    sections = [loops, state_map, input_map, value_matrix, feedback, gain_inverse]
    rows = [
        states, inputs, multipliers, bound_mult, upper_bound, offset, state_weight, state_linear, input_linear,
        input_weight,
    ]
    kept = sections + rows
    out = pl.pallas_call(
        functools.partial(block_product_body, sections=sections, rows=len(rows)),
        in_specs=[pl.BlockSpec(memory_space=pltpu.HBM)] * len(kept),
        out_specs=[FULL] * (4 + len(kept)),
        out_shape=[in_vmem(o) for o in [(256, 256), (4, 256, 256), (4, 256, 256), (256, 256)] + [k.shape for k in kept]],
        scratch_shapes=[room(4, 256, 256), pltpu.SemaphoreType.DMA((3 + len(kept),))],
        compiler_params=pltpu.CompilerParams(vmem_limit_bytes=24 * 1024 * 1024),
        name="block_product",
    )(*[pltpu.with_memory_space_constraint(k, pltpu.HBM) for k in kept])
    product, pairs, quads, half = out[:4]
    loop_v, map_v, push_v, value_v, feed_v, inverse_v = out[4:10]
    rows_v = out[10:]

    defect, grad_input, sources, inner, block, statistics = call(
        sources_body, [],
        [], [],
        [map_v, push_v, value_v, feed_v, loop_v, *rows_v, quads, half, product, from_before, from_after],
        [(16, 256), (16, 64), (16, 256), (16, 256), (264, 256), (8, 128)],
        [room(16, 256)],
    )
    near_z = turned(block, "tm_2")

    def join(axis, *parts):
        return call(
            functools.partial(join_body, axis=axis), [place], [], [],
            list(parts),
            [(4, 256, 256), (4, 8, 256), (264, 256)], [],
        )

    pairs, block = lax.optimization_barrier((pairs, block))
    weight, third = call(
        weight_body, [], [], [], [loop_v, push_v, inverse_v, pairs, quads, half],
        [(256, 256), (256, 256)], [room(1024, 256), room(1024, 256)],
    )
    near_z, weight, third = lax.optimization_barrier((near_z, weight, third))
    maps_z, vectors_z, group = join(2, block, *near_z)
    near_x = turned(group, "tm_1")

    inner, group = lax.optimization_barrier((inner, group))
    (local_state,) = call(
        local_body, [], [], [],
        [loop_v, push_v, inverse_v, quads, inner, sources, grad_input, defect],
        [(8, 256)],
        [room(16, 256), room(16, 64), room(16, 64), room(16, 256), room(16, 256)],
    )
    near_x, local_state = lax.optimization_barrier((near_x, local_state))
    maps_x, vectors_x, plane = join(1, group, *near_x)
    near_y = turned(plane, "tm_0")

    maps_x, plane = lax.optimization_barrier((maps_x, plane))
    rest_z, rest, constant, until_z, until = call(
        compose_body, [place], [], [], [maps_x, vectors_x, maps_z, vectors_z],
        [(256, 256), (256, 256), (8, 256), (256, 256), (256, 256)], [],
    )

    incoming, message = call(
        costate_body, [place], [], [],
        [plane, *near_y, rest_z, rest, constant, weight, local_state, statistics],
        [(8, 256), (64, 1, 384)], [room(4, 256, 256), room(4, 8, 256)], away=(0, 1),
    )

    received = lax.all_to_all(message, TM, 0, 0, tiled=True)

    before, gain, base, push, entry = call(
        sweep_body, [], [part(quads), part(closed_loop, 1), part(input_map, 1), part(gain_inverse, 1)],
        [inner, sources, grad_input, defect, incoming], [],
        [(16, 256), (16, 64), (16, 64), (16, 256), (8, 256)], [room(16, 256)], away=range(5),
    )

    state_step, input_step, multiplier_step, bound_step, sums = call(
        functools.partial(finish_body, horizon=states.shape[0] * lax.axis_size(TM)), [place],
        [part(a) for a in (plane, *near_y)]
        + [part(a, 0, 1, 1, 2) for a in (maps_x, maps_z)]
        + [part(until_z), part(until), part(quads, 0, 1, 0, 1), part(half), part(third)]
        + [part(closed_loop, 1), part(value_matrix, 2), part(feedback, 2)],
        [active, upper_bound, inputs, input_weight, defect, before, gain, base, push, entry],
        [received],
        [(16, 256), (16, 64), (16, 256), (16, 64), (1, 3)],
        [room(4, 256, 256)], final=True,
    )

    kkt_norms = sums.reshape(3)
    return (state_step, input_step, multiplier_step, bound_step, kkt_norms)


def solution(mesh):
    split = Mesh(
        mesh.devices.reshape(4, 4, 4, mesh.shape["batch"]), ("tm_0", "tm_1", "tm_2", "batch")
    )

    return jax.shard_map(
        local,
        mesh=split,
        in_specs=(P(BATCH_TM, None, None),) * 6 + (P("batch", None),) + (P(BATCH_TM, None),) * 10,
        out_specs=(P(BATCH_TM, None),) * 4 + (P("batch"),),
        check_vma=False,
    )
```
